32 devices in a mesh: member: 2 (over x), wave: 16 (over z, y, core).
Axes of the slice: x: 2, y: 2, z: 4, core: 2. Of those that a mesh axis runs over, the one named last changes fastest.
Arguments:
- vorticity: bfloat16 [2560, 32, 1280], P(('member', 'wave')), parts along dimension 0, may hold values from -6 to 6
- divergence: bfloat16 [2560, 32, 1280], P(('member', 'wave')), parts along dimension 0, may hold values from -6 to 6
- legendre: bfloat16 [1280, 16, 1280], P('wave'), may hold values from -0.0068359375 to 0.0068359375
- wave_of_slot: int32 [1280], replicated, may hold values from 0 to 1279, as said below
- cycle_points: int32 [16], P('wave'), may hold values from 20 to 5136, as said below
- cos_squared: float32 [16], P('wave'), may hold values from 0.25 to 1
Outputs:
- grid: bfloat16 [32, 96, 5136], P(('member', 'wave')), parts along dimension 0
The draws below stay inside these ranges and needn't reach their ends.
There are 2 independent parts, one for each index of `member`. The reference program is written for one: setup_inputs(seed, part) draws one part's arguments, and reference() takes and returns one part's arrays. A program takes and returns all parts, laid end to end along the dimension named above; an argument that names none is the same for every part. Nothing has to cross between parts.
Inputs may be any that keep to these rules, and one draw needn't show every extreme that they name: `wave_of_slot`: each wavenumber appears in exactly one slot. `cycle_points`: every count is a multiple of 4; some cycle has 5136 points.
All inputs are finite; a program needn't handle non-finite values.
Results may differ from the reference program's by a relative error of at most 0.0063.
Values may be sent and summed in bfloat16 or wider, within the bound.
A program may use at most 192 MiB of HBM per device.

```python
import jax
import jax.numpy as jnp
from jax import lax

NWAVE = 1280
LEV = 16
NLON = 5136
NLAT_WIN = 16


def draw_wave_of_slot(key, part):
    return jax.random.permutation(key, NWAVE).astype(jnp.int32)


def draw_cycle_points(key, part):
    key_steps, key_place = jax.random.split(key)
    counts = jax.random.randint(key_steps, (NLAT_WIN,), 0, (NLON - 20) // 4 + 1, dtype=jnp.int32)
    widest = jax.random.randint(key_place, (), 0, NLAT_WIN, dtype=jnp.int32)
    based = 20 + 4 * counts
    return jnp.where(jnp.arange(NLAT_WIN, dtype=jnp.int32) == widest, NLON, based).astype(jnp.int32)


def level_of(key, extent, cuts, least, largest):
    gain, own = 1.0, jax.random.fold_in(key, 6)
    for dim, shards_of in cuts:
        draws = jnp.exp(jax.random.uniform(jax.random.fold_in(own, dim), (shards_of,), jnp.float32, least / len(cuts), largest / len(cuts)))
        gain = gain * jnp.repeat(draws, extent[dim] // shards_of).reshape([-1 if axis == dim else 1 for axis in range(len(extent))])
    return gain


def noise(own_key, extent, spread, bound, cuts=(), held_as=jnp.bfloat16):
    result = jax.random.normal(own_key, extent, jnp.float32) * spread
    if len(cuts) > 0:
        result = level_of(own_key, extent, cuts, -0.22, 0.18) * result
    return jnp.clip(result, min=-bound, max=bound).astype(held_as)


def setup_inputs(seed: int = 0, part: int = 0) -> dict:
    key_of = jax.random.split(jax.random.key(seed), 7)
    own_keys = jax.random.split(jax.random.fold_in(key_of[6], part), 7)
    vorticity = noise(own_keys[0], (NWAVE, 2 * LEV, NWAVE), 1.0, 6.0, ((0, 16),))
    divergence = noise(own_keys[1], (NWAVE, 2 * LEV, NWAVE), 1.0, 6.0, ((0, 16),))
    legendre = noise(key_of[2], (NWAVE, NLAT_WIN, NWAVE), (NWAVE * NWAVE // 2) ** -0.5, 0.0068359375, ((0, 16),))
    wave_of_slot = draw_wave_of_slot(jax.random.fold_in(key_of[6], 71), part)
    cycle_points = draw_cycle_points(jax.random.fold_in(key_of[6], 71), part)
    cos_squared = jnp.clip(0.25 + 0.75 * jax.random.uniform(key_of[5], (NLAT_WIN,), jnp.float32) ** level_of(key_of[5], (NLAT_WIN,), ((0, 16),), -0.2, 0.2), 0.25, 1.0)
    return dict(vorticity=vorticity, divergence=divergence, legendre=legendre, wave_of_slot=wave_of_slot, cycle_points=cycle_points, cos_squared=cos_squared)


def spectral_fields(zeta_in, delta_in, waves):
    columns = zeta_in.shape[-1]
    levels = zeta_in.shape[1] // 2
    degree = waves[:, None] + jnp.arange(columns, dtype=jnp.int32)[None, :]
    living = degree < NWAVE
    positive = living & (degree > 0)
    wave_f = waves.astype(jnp.float32)[:, None]
    degree_f = degree.astype(jnp.float32)
    radius = NWAVE / 4.0
    inverse = jnp.where(positive, -radius / jnp.maximum(degree_f * (degree_f + 1.0), 1.0), 0.0)
    quotient = jnp.maximum(degree_f * degree_f - wave_f * wave_f, 0.0) / jnp.maximum(4.0 * degree_f * degree_f - 1.0, 1.0)
    coupling = jnp.where(positive, jnp.sqrt(quotient), 0.0)
    coupling_next = jnp.concatenate([coupling[:, 1:], jnp.zeros_like(coupling[:, :1])], axis=1)
    upper_coef = ((degree_f + 2.0) * coupling_next)[:, None, :]
    lower_coef = ((degree_f - 1.0) * coupling)[:, None, :]
    live_mask = living.astype(jnp.float32)[:, None, :]
    zeta = zeta_in.astype(jnp.float32) * live_mask
    delta = delta_in.astype(jnp.float32) * live_mask
    stream = zeta * inverse[:, None, :]
    potential = delta * inverse[:, None, :]

    def meridional(values):
        shifted_up = jnp.concatenate([values[..., 1:], jnp.zeros_like(values[..., :1])], axis=-1)
        shifted_down = jnp.concatenate([jnp.zeros_like(values[..., :1]), values[..., :-1]], axis=-1)
        return (upper_coef * shifted_up - lower_coef * shifted_down) * live_mask
    stream_h = meridional(stream)
    potential_h = meridional(potential)
    wave_three = waves.astype(jnp.float32)[:, None, None]
    u_real = -wave_three * potential[:, levels:] - stream_h[:, :levels]
    u_imag = wave_three * potential[:, :levels] - stream_h[:, levels:]
    v_real = -wave_three * stream[:, levels:] + potential_h[:, :levels]
    v_imag = wave_three * stream[:, :levels] + potential_h[:, levels:]
    return jnp.concatenate([u_real, u_imag, v_real, v_imag, zeta, delta], axis=1).astype(jnp.bfloat16)

def derive(fourier, waves, cosine_sq):
    cycles, slots, columns = fourier.shape
    levels = columns // 8
    groups = fourier.reshape(cycles, slots, 4, 2, levels)
    wind_u = groups[:, :, 0]
    wind_v = groups[:, :, 1]
    zeta_f = groups[:, :, 2]
    delta_f = groups[:, :, 3]
    scale = (waves.astype(jnp.float32) / (NWAVE / 4.0))[None, :, None]
    u_lon = jnp.stack([-scale * wind_u[:, :, 1], scale * wind_u[:, :, 0]], axis=2)
    v_lon = jnp.stack([-scale * wind_v[:, :, 1], scale * wind_v[:, :, 0]], axis=2)
    factor = cosine_sq[:, None, None, None]
    u_lat = v_lon / factor - zeta_f
    v_lat = delta_f - u_lon / factor
    stacked = jnp.stack([wind_u, wind_v, u_lon, v_lon, u_lat, v_lat], axis=2)
    return stacked.reshape(cycles, slots, 12 * levels)

def cycle_basis(waves, points):
    positions = jnp.arange(NLON, dtype=jnp.int32)
    phase = waves[:, None] * positions[None, :] % points
    theta = 2.0 * jnp.pi / points.astype(jnp.float32) * phase.astype(jnp.float32)
    keeping = (2 * waves[:, None] < points) & (positions[None, :] < points)
    weight = jnp.where(waves == 0, 1.0, 2.0)[:, None]
    cosine = jnp.where(keeping, weight * jnp.cos(theta), 0.0)
    sine = jnp.where(keeping, -weight * jnp.sin(theta), 0.0)
    return jnp.stack([cosine, sine]).astype(jnp.bfloat16)

def reference(vorticity, divergence, legendre, wave_of_slot, cycle_points, cos_squared):
    blocks = NWAVE // 16

    def block_fourier(item):
        zeta_in, delta_in, values, waves = item
        spec = spectral_fields(zeta_in, delta_in, waves)
        return jnp.einsum('sck,slk->lsc', spec.astype(jnp.float32), values.astype(jnp.float32))
    items = (vorticity.reshape(blocks, 16, 2 * LEV, NWAVE), divergence.reshape(blocks, 16, 2 * LEV, NWAVE), legendre.reshape(blocks, 16, NLAT_WIN, NWAVE), wave_of_slot.reshape(blocks, 16))
    mapped = lax.map(block_fourier, items)
    fourier = jnp.transpose(mapped, (1, 0, 2, 3)).reshape(NLAT_WIN, NWAVE, 8 * LEV)
    fields = derive(fourier, wave_of_slot, cos_squared)

    def one_cycle(item):
        cycle_fields, points = item
        packed = cycle_fields.astype(jnp.bfloat16).reshape(NWAVE, 6, 2, LEV).astype(jnp.float32)
        basis = cycle_basis(wave_of_slot, points).astype(jnp.float32)
        summed = jnp.einsum('sfrl,rsp->flp', packed, basis)
        return summed.reshape(6 * LEV, NLON).astype(jnp.bfloat16)
    return lax.map(one_cycle, (fields, cycle_points))
```

```python
import functools

import jax
import jax.numpy as jnp
from jax import lax
from jax.experimental import pallas as pl
from jax.experimental.pallas import tpu as pltpu
from jax.sharding import PartitionSpec as P

NLON = 5136
LANES = 128
COS = (1.0, -1 / 2, 1 / 24, -1 / 720, 1 / 40320, -1 / 3628800, 1 / 479001600,
       -1 / 87178291200, 1 / 20922789888000, -1 / 6402373705728000)
SIN = (1.0, -1 / 6, 1 / 120, -1 / 5040, 1 / 362880, -1 / 39916800, 1 / 6227020800,
       -1 / 1307674368000, 1 / 355687428096000, -1 / 121645100408832000)


def slot_block(slots):
    return max(b for b in range(1, 17) if slots % b == 0)


def degree_coefs(wave, count):
    column = lax.broadcasted_iota(jnp.int32, (wave.shape[0], count), 1)
    degree = wave + column
    living = degree < count
    positive = living & (degree > 0)
    m = wave.astype(jnp.float32)
    n = degree.astype(jnp.float32)
    radius = count / 4.0
    square = n * n
    ratio = jnp.maximum(square - m * m, 0.0) / jnp.maximum(square * (4.0 * square - 1.0), 1.0)
    lower = radius * jnp.sqrt(ratio)
    upper = pltpu.roll(lower, count - 1, 1)
    along = jnp.where(positive, -radius * m / jnp.maximum(n * (n + 1.0), 1.0), 0.0)
    before = jnp.where(positive, -lower, 0.0)
    after = jnp.where((degree > 0) & (degree + 1 < count), upper, 0.0)
    return living.astype(jnp.float32), along, before, after


def slot_fourier(values, live, along, before, after, zd):
    count = values.shape[-1]
    p = values.astype(jnp.float32)
    lon = p * along
    lat = pltpu.roll(p, 1, 1) * before + pltpu.roll(p, count - 1, 1) * after
    left = jnp.concatenate([p * live, lon, lat], axis=0).astype(jnp.bfloat16)
    sums = lax.dot_general(left, zd, (((1,), (1,)), ((), ())), preferred_element_type=jnp.float32)
    rows = p.shape[0]
    lev = zd.shape[0] // 4
    plain, a, b = sums[:rows], sums[rows : 2 * rows], sums[2 * rows :]
    zr, zi, dr, di = (slice(g * lev, (g + 1) * lev) for g in range(4))
    turned = jnp.concatenate([-a[:, di], a[:, dr], -a[:, zi], a[:, zr]], axis=1)
    lane = lax.broadcasted_iota(jnp.int32, b.shape, 1)
    winds = turned + jnp.where(lane < 2 * lev, -b, b)
    return jnp.concatenate([winds, plain], axis=1)


def horner(coefs, x):
    total = jnp.full_like(x, coefs[-1])
    for c in coefs[-2::-1]:
        total = total * x + c
    return total


def turn(steps, points, per_point):
    turns = jnp.round(steps * per_point)
    theta = (steps - turns * points) * (per_point * (2.0 * jnp.pi))
    square = theta * theta
    return horner(COS, square), theta * horner(SIN, square)


def columns_of(row):
    return jnp.broadcast_to(row, (LANES, row.shape[1])).T


def fill_basis(wave_col, steps, points, basis):
    step_c, step_s = (columns_of(x) for x in steps)
    slots = wave_col.shape[0]
    lane = lax.broadcasted_iota(jnp.int32, (16, LANES), 1).astype(jnp.float32)
    for start in range(0, slots, 16):
        rows = slice(start, start + 16)
        c, s = turn(wave_col[rows] * lane, points, 1.0 / points)
        cs, ss = step_c[rows], step_s[rows]
        for t in range(basis.shape[1] // LANES):
            at = slice(t * LANES, (t + 1) * LANES)
            basis[rows, at] = c.astype(basis.dtype)
            basis[slots + start : slots + start + 16, at] = s.astype(basis.dtype)
            c, s = c * cs - s * ss, s * cs + c * ss


def fill_fields(arrived, wave, points, cosine_sq, count, packed):
    x = arrived.astype(jnp.float32).T
    lev = x.shape[0] // 8
    ur, ui, vr, vi, zr, zi, dr, di = (x[g * lev : (g + 1) * lev] for g in range(8))
    slots = wave.shape[1]
    m = wave.astype(jnp.float32)
    q = m * (4.0 / count)
    over = 1.0 / jnp.full_like(m, cosine_sq)
    ulr, uli, vlr, vli = -q * ui, q * ur, -q * vi, q * vr
    fields = (
        (ur, ui), (vr, vi), (ulr, uli), (vlr, vli),
        (vlr * over - zr, vli * over - zi), (dr - ulr * over, di - uli * over),
    )
    weight = jnp.where(2 * wave < points, jnp.where(wave == 0, 1.0, 2.0), 0.0)
    parity = jnp.where((wave & 1) == 0, 1.0, -1.0)
    half = len(fields) * lev
    for f, (re, im) in enumerate(fields):
        for part, x in enumerate((re * weight, -im * weight)):
            packed[part, f * lev : (f + 1) * lev] = x.astype(packed.dtype)
            packed[part, half + f * lev : half + (f + 1) * lev] = (x * parity).astype(packed.dtype)


def send_groups(blocks):
    return [(b, b + 1) for b in range(blocks)]


def partners(me, devices):
    if devices % 2:
        return [lax.rem(me + off, devices) for off in range(1, devices)]
    half = devices // 2
    side = me // half
    far = [(1 - side) * half + lax.rem(me + off, half) for off in range(half)]
    near = [side * half + lax.rem(me + off, half) for off in range(1, half)]
    return far + near


def exchange_kernel(
    groups, points_ref, cosine_ref, wave_hbm, zeta_hbm, delta_hbm, values_hbm, quarters_ref,
    wave_ref, wave_col, zeta_ref, delta_ref, values_ref, sums, sent, held, basis, packed,
    wave_sem, in_sem, send_sem, recv_sem,
):
    cycles, devices, blocks, sb, columns = held.shape
    count = zeta_ref.shape[-1]
    rows = values_ref.shape[1]
    me = lax.axis_index("wave")
    barrier = pltpu.get_barrier_semaphore()
    peers = partners(me, devices)

    def fetch(step):
        at = pl.ds(step * sb, sb)
        return [
            pltpu.make_async_copy(source.at[at], target.at[at], in_sem.at[k, step])
            for k, (source, target) in enumerate(
                ((zeta_hbm, zeta_ref), (delta_hbm, delta_ref), (values_hbm, values_ref))
            )
        ]

    load_wave = pltpu.make_async_copy(wave_hbm, wave_ref, wave_sem)
    load_wave.start()
    for step in range(blocks):
        for copy in fetch(step):
            copy.start()
    for to in peers:
        pl.semaphore_signal(
            barrier, inc=1, device_id={"wave": to}, device_id_type=pl.DeviceIdType.MESH
        )

    def send(group):
        start, stop = groups[group]
        for to in peers:
            for cycle in range(cycles):
                pltpu.make_async_remote_copy(
                    src_ref=sent.at[to * cycles + cycle, start:stop],
                    dst_ref=held.at[cycle, me, start:stop],
                    send_sem=send_sem.at[cycle],
                    recv_sem=recv_sem.at[cycle],
                    device_id={"wave": to},
                    device_id_type=pl.DeviceIdType.MESH,
                ).start()

    load_wave.wait()
    wave = wave_ref[...].reshape(1, -1)
    slots = wave.shape[1]
    wave_f = wave.astype(jnp.float32)
    wave_col[...] = columns_of(wave_f)

    def legendre(step, carry):
        for copy in fetch(step):
            copy.wait()
        waves = wave_col[pl.ds(me * (blocks * sb) + step * sb, sb), 0:1].astype(jnp.int32)
        coefs = degree_coefs(waves, count)
        for s in range(sb):
            slot = step * sb + s
            zd = jnp.concatenate([zeta_ref[slot], delta_ref[slot]], axis=0)
            out = slot_fourier(values_ref[slot], *(c[s : s + 1] for c in coefs), zd)
            sums[pl.ds(s, rows, sb), :] = out
        sent[:, step] = sums[...].astype(sent.dtype).reshape(rows, sb, columns)
        for cycle in range(cycles):
            mine = sums[pl.ds((me * cycles + cycle) * sb, sb), :]
            held[cycle, me, step] = mine.astype(held.dtype)
        for group, (_, stop) in enumerate(groups):
            @pl.when(step == stop - 1)
            def _():
                if group == 0:
                    pl.semaphore_wait(barrier, devices - 1)
                send(group)
        return carry

    lax.fori_loop(0, blocks, legendre, 0)
    for cycle in range(cycles):
        points = points_ref[cycle]
        points_f = jnp.full((1, 1), points, jnp.int32).astype(jnp.float32)
        steps = turn(wave_f * float(LANES), points_f, 1.0 / points_f)
        fill_basis(wave_col, steps, points_f, basis)
        others = held.at[cycle, 0 : devices - 1]
        if cycle == 0:
            for c in range(cycles):
                all_of = held.at[c, 0 : devices - 1]
                pltpu.make_async_copy(all_of, all_of, recv_sem.at[c]).wait()
        arrived = held[cycle].reshape(slots, columns)
        fill_fields(arrived, wave, points, cosine_ref[cycle], count, packed)
        width = basis.shape[1]
        half = packed.shape[1] // 2
        for start in range(0, width, 256):
            at = slice(start, min(start + 256, width))
            cosine, sine = (
                jnp.dot(
                    packed[part], basis[part * slots : (part + 1) * slots, at],
                    preferred_element_type=jnp.float32,
                )
                for part in range(2)
            )
            parts = (
                cosine[:half] + sine[:half], cosine[half:] - sine[half:],
                cosine[half:] + sine[half:], cosine[:half] - sine[:half],
            )
            for j, x in enumerate(parts):
                quarters_ref[cycle, j * half : (j + 1) * half, at] = x.astype(quarters_ref.dtype)
        pltpu.make_async_copy(others, others, send_sem.at[cycle]).wait()


def basis_width():
    return -(-(NLON // 4 + 1) // LANES) * LANES


def cycle_quarters(points, cosine_sq, wave_of_slot, vorticity, divergence, legendre):
    slots, half, count = vorticity.shape
    lines = legendre.shape[1]
    cycles = points.shape[0]
    devices = lines // cycles
    columns = 4 * half
    rows = 6 * half
    width = basis_width()
    sb = slot_block(slots)
    blocks = slots // sb
    smem = pl.BlockSpec(memory_space=pltpu.SMEM)
    hbm = pl.BlockSpec(memory_space=pltpu.HBM)
    sem = pltpu.SemaphoreType.DMA((cycles,))
    return pl.pallas_call(
        functools.partial(exchange_kernel, send_groups(blocks)),
        in_specs=[smem, smem, hbm, hbm, hbm, hbm],
        out_specs=pl.BlockSpec(memory_space=pltpu.VMEM),
        out_shape=jax.ShapeDtypeStruct((cycles, 2 * rows, width), jnp.bfloat16),
        scratch_shapes=[
            pltpu.VMEM(wave_of_slot.shape, jnp.int32),
            pltpu.VMEM((devices * slots, LANES), jnp.float32),
            pltpu.VMEM(vorticity.shape, vorticity.dtype),
            pltpu.VMEM(divergence.shape, divergence.dtype),
            pltpu.VMEM(legendre.shape, legendre.dtype),
            pltpu.VMEM((lines * sb, columns), jnp.float32),
            pltpu.VMEM((lines, blocks, sb, columns), jnp.bfloat16),
            pltpu.VMEM((cycles, devices, blocks, sb, columns), jnp.bfloat16),
            pltpu.VMEM((2 * devices * slots, width), jnp.bfloat16),
            pltpu.VMEM((2, rows, devices * slots), jnp.bfloat16),
            pltpu.SemaphoreType.DMA,
            pltpu.SemaphoreType.DMA((3, blocks)),
            sem,
            sem,
        ],
        compiler_params=pltpu.CompilerParams(
            collective_id=0, has_side_effects=True, vmem_limit_bytes=40 << 20
        ),
    )(points, cosine_sq, wave_of_slot, vorticity, divergence, legendre)


def place(quarters, points, line):
    rows = quarters.shape[0] // 4
    width = quarters.shape[1]
    tiles = width // LANES
    quarter = points // 4
    lane = lax.broadcasted_iota(jnp.int32, (rows, LANES), 1)
    line[...] = jnp.zeros_like(line)
    for j in range(4):
        turned = j % 2
        offset = quarter * (j + 1) - (width - 1) if turned else quarter * j
        offset = offset + front_lanes(width)
        base = pl.multiple_of(offset // LANES * LANES, LANES)
        shift = offset - base
        source = lane - shift if not turned else shift - 1 - lane
        source = source & (LANES - 1)
        previous = jnp.zeros((rows, LANES), jnp.float32)
        for t in range(tiles + 1):
            rolled = jnp.zeros((rows, LANES), jnp.float32)
            if t < tiles:
                u = tiles - 1 - t if turned else t
                tile = quarters[j * rows : (j + 1) * rows, u * LANES : (u + 1) * LANES]
                point = lane + u * LANES
                keep = (point > 0) & (point <= quarter) if turned else point < quarter
                tile = jnp.where(keep, tile.astype(jnp.float32), 0.0)
                rolled = jnp.take_along_axis(tile, source, axis=1)
            moved = jnp.where(lane < shift, previous, rolled).astype(line.dtype)
            at = pl.ds(pl.multiple_of(base + t * LANES, LANES), LANES)
            line[:, at] = line[:, at] + moved
            previous = rolled


def front_lanes(width):
    return width + LANES


def place_kernel(points_ref, quarters_ref, out_ref, line):
    place(quarters_ref.at[0], points_ref[pl.program_id(0)], line)
    front = front_lanes(quarters_ref.shape[2])
    out_ref[0] = line[:, front : front + out_ref.shape[2]]


def placed(quarters, points):
    cycles, rows, width = quarters.shape
    rows = rows // 4
    line = front_lanes(width) + 4 * width + 2 * LANES
    return pl.pallas_call(
        place_kernel,
        grid=(cycles,),
        in_specs=[
            pl.BlockSpec(memory_space=pltpu.SMEM),
            pl.BlockSpec((1, 4 * rows, width), lambda i: (i, 0, 0)),
        ],
        out_specs=pl.BlockSpec((1, rows, NLON), lambda i: (i, 0, 0)),
        out_shape=jax.ShapeDtypeStruct((cycles, rows, NLON), jnp.bfloat16),
        scratch_shapes=[pltpu.VMEM((rows, line), jnp.bfloat16)],
        compiler_params=pltpu.CompilerParams(vmem_limit_bytes=16 << 20),
    )(points, quarters)


def body(vorticity, divergence, legendre, wave_of_slot, cycle_points, cos_squared):
    quarters = cycle_quarters(
        cycle_points, cos_squared, wave_of_slot, vorticity, divergence, legendre
    )
    return placed(quarters, cycle_points)


def solution(mesh):
    return jax.shard_map(
        body,
        mesh=mesh,
        in_specs=(
            P(("member", "wave"), None, None),
            P(("member", "wave"), None, None),
            P("wave", None, None),
            P(),
            P("wave"),
            P("wave"),
        ),
        out_specs=P(("member", "wave"), None, None),
        check_vma=False,
    )
```

```python
import functools

import jax
import jax.numpy as jnp
from jax import lax
from jax.experimental import pallas as pl
from jax.experimental.pallas import tpu as pltpu
from jax.sharding import PartitionSpec as P

NLON = 5136
LANES = 128
COS = (1.0, -1 / 2, 1 / 24, -1 / 720, 1 / 40320, -1 / 3628800, 1 / 479001600,
       -1 / 87178291200, 1 / 20922789888000, -1 / 6402373705728000)
SIN = (1.0, -1 / 6, 1 / 120, -1 / 5040, 1 / 362880, -1 / 39916800, 1 / 6227020800,
       -1 / 1307674368000, 1 / 355687428096000, -1 / 121645100408832000)


def slot_block(slots):
    return max(b for b in range(1, 17) if slots % b == 0)


def degree_coefs(wave, count):
    column = lax.broadcasted_iota(jnp.int32, (wave.shape[0], count), 1)
    degree = wave + column
    living = degree < count
    positive = living & (degree > 0)
    m = wave.astype(jnp.float32)
    n = degree.astype(jnp.float32)
    radius = count / 4.0
    square = n * n
    ratio = jnp.maximum(square - m * m, 0.0) / jnp.maximum(square * (4.0 * square - 1.0), 1.0)
    lower = radius * jnp.sqrt(ratio)
    upper = pltpu.roll(lower, count - 1, 1)
    along = jnp.where(positive, -radius * m / jnp.maximum(n * (n + 1.0), 1.0), 0.0)
    before = jnp.where(positive, -lower, 0.0)
    after = jnp.where((degree > 0) & (degree + 1 < count), upper, 0.0)
    return living.astype(jnp.float32), along, before, after


def slot_fourier(values, live, along, before, after, zd):
    count = values.shape[-1]
    p = values.astype(jnp.float32)
    lon = p * along
    lat = pltpu.roll(p, 1, 1) * before + pltpu.roll(p, count - 1, 1) * after
    left = jnp.concatenate([p * live, lon, lat], axis=0).astype(jnp.bfloat16)
    sums = lax.dot_general(left, zd, (((1,), (1,)), ((), ())), preferred_element_type=jnp.float32)
    rows = p.shape[0]
    lev = zd.shape[0] // 4
    plain, a, b = sums[:rows], sums[rows : 2 * rows], sums[2 * rows :]
    zr, zi, dr, di = (slice(g * lev, (g + 1) * lev) for g in range(4))
    turned = jnp.concatenate([-a[:, di], a[:, dr], -a[:, zi], a[:, zr]], axis=1)
    lane = lax.broadcasted_iota(jnp.int32, b.shape, 1)
    winds = turned + jnp.where(lane < 2 * lev, -b, b)
    return jnp.concatenate([winds, plain], axis=1)


def horner(coefs, x):
    total = jnp.full_like(x, coefs[-1])
    for c in coefs[-2::-1]:
        total = total * x + c
    return total


def turn(steps, points, per_point):
    turns = jnp.round(steps * per_point)
    theta = (steps - turns * points) * (per_point * (2.0 * jnp.pi))
    square = theta * theta
    return horner(COS, square), theta * horner(SIN, square)


def columns_of(row):
    return jnp.broadcast_to(row, (LANES, row.shape[1])).T


def fill_basis(wave_col, steps, points, basis):
    step_c, step_s = (columns_of(x) for x in steps)
    slots = wave_col.shape[0]
    lane = lax.broadcasted_iota(jnp.int32, (16, LANES), 1).astype(jnp.float32)
    for start in range(0, slots, 16):
        rows = slice(start, start + 16)
        c, s = turn(wave_col[rows] * lane, points, 1.0 / points)
        cs, ss = step_c[rows], step_s[rows]
        for t in range(basis.shape[1] // LANES):
            at = slice(t * LANES, (t + 1) * LANES)
            basis[rows, at] = c.astype(basis.dtype)
            basis[slots + start : slots + start + 16, at] = s.astype(basis.dtype)
            c, s = c * cs - s * ss, s * cs + c * ss


def fill_fields(arrived, wave, points, cosine_sq, count, packed):
    x = arrived.astype(jnp.float32).T
    lev = x.shape[0] // 8
    ur, ui, vr, vi, zr, zi, dr, di = (x[g * lev : (g + 1) * lev] for g in range(8))
    slots = wave.shape[1]
    m = wave.astype(jnp.float32)
    q = m * (4.0 / count)
    over = 1.0 / jnp.full_like(m, cosine_sq)
    ulr, uli, vlr, vli = -q * ui, q * ur, -q * vi, q * vr
    fields = (
        (ur, ui), (vr, vi), (ulr, uli), (vlr, vli),
        (vlr * over - zr, vli * over - zi), (dr - ulr * over, di - uli * over),
    )
    weight = jnp.where(2 * wave < points, jnp.where(wave == 0, 1.0, 2.0), 0.0)
    parity = jnp.where((wave & 1) == 0, 1.0, -1.0)
    half = len(fields) * lev
    for f, (re, im) in enumerate(fields):
        for part, x in enumerate((re * weight, -im * weight)):
            packed[part, f * lev : (f + 1) * lev] = x.astype(packed.dtype)
            packed[part, half + f * lev : half + (f + 1) * lev] = (x * parity).astype(packed.dtype)


def send_groups(blocks):
    return [(b, b + 1) for b in range(blocks)]


def partners(me, devices):
    if devices % 2:
        return [lax.rem(me + off, devices) for off in range(1, devices)]
    half = devices // 2
    side = me // half
    far = [(1 - side) * half + lax.rem(me + off, half) for off in range(half)]
    near = [side * half + lax.rem(me + off, half) for off in range(1, half)]
    return far + near


def exchange_kernel(
    groups, points_ref, cosine_ref, wave_hbm, zeta_hbm, delta_hbm, values_hbm, quarters_ref,
    wave_ref, wave_col, zeta_ref, delta_ref, values_ref, sums, sent, held, basis, packed,
    wave_sem, in_sem, send_sem, recv_sem,
):
    cycles, devices, blocks, sb, columns = held.shape
    count = zeta_ref.shape[-1]
    rows = values_ref.shape[1]
    me = lax.axis_index("wave")
    barrier = pltpu.get_barrier_semaphore()
    peers = partners(me, devices)

    def fetch(step):
        at = pl.ds(step * sb, sb)
        return [
            pltpu.make_async_copy(source.at[at], target.at[at], in_sem.at[k, step])
            for k, (source, target) in enumerate(
                ((zeta_hbm, zeta_ref), (delta_hbm, delta_ref), (values_hbm, values_ref))
            )
        ]

    load_wave = pltpu.make_async_copy(wave_hbm, wave_ref, wave_sem)
    load_wave.start()
    def start(step):
        for copy in fetch(step):
            copy.start()

    start(0)
    for to in peers:
        pl.semaphore_signal(
            barrier, inc=1, device_id={"wave": to}, device_id_type=pl.DeviceIdType.MESH
        )

    def send(group):
        start, stop = groups[group]
        for to in peers:
            for cycle in range(cycles):
                pltpu.make_async_remote_copy(
                    src_ref=sent.at[to * cycles + cycle, start:stop],
                    dst_ref=held.at[cycle, me, start:stop],
                    send_sem=send_sem.at[cycle],
                    recv_sem=recv_sem.at[cycle],
                    device_id={"wave": to},
                    device_id_type=pl.DeviceIdType.MESH,
                ).start()

    load_wave.wait()
    if blocks > 1:
        start(1)
    wave = wave_ref[...].reshape(1, -1)
    slots = wave.shape[1]
    wave_f = wave.astype(jnp.float32)
    wave_col[...] = columns_of(wave_f)

    def legendre(step, carry):
        for copy in fetch(step):
            copy.wait()
        pl.when(step + 2 < blocks)(lambda: start(step + 2))
        waves = wave_col[pl.ds(me * (blocks * sb) + step * sb, sb), 0:1].astype(jnp.int32)
        coefs = degree_coefs(waves, count)
        for s in range(sb):
            slot = step * sb + s
            zd = jnp.concatenate([zeta_ref[slot], delta_ref[slot]], axis=0)
            out = slot_fourier(values_ref[slot], *(c[s : s + 1] for c in coefs), zd)
            sums[pl.ds(s, rows, sb), :] = out
        sent[:, step] = sums[...].astype(sent.dtype).reshape(rows, sb, columns)
        for cycle in range(cycles):
            mine = sums[pl.ds((me * cycles + cycle) * sb, sb), :]
            held[cycle, me, step] = mine.astype(held.dtype)
        for group, (_, stop) in enumerate(groups):
            @pl.when(step == stop - 1)
            def _():
                if group == 0:
                    pl.semaphore_wait(barrier, devices - 1)
                send(group)
        return carry

    lax.fori_loop(0, blocks, legendre, 0)
    for cycle in range(cycles):
        points = points_ref[cycle]
        points_f = jnp.full((1, 1), points, jnp.int32).astype(jnp.float32)
        steps = turn(wave_f * float(LANES), points_f, 1.0 / points_f)
        fill_basis(wave_col, steps, points_f, basis)
        others = held.at[cycle, 0 : devices - 1]
        if cycle == 0:
            for c in range(cycles):
                all_of = held.at[c, 0 : devices - 1]
                pltpu.make_async_copy(all_of, all_of, recv_sem.at[c]).wait()
        arrived = held[cycle].reshape(slots, columns)
        fill_fields(arrived, wave, points, cosine_ref[cycle], count, packed)
        width = basis.shape[1]
        half = packed.shape[1] // 2
        for start in range(0, width, 256):
            at = slice(start, min(start + 256, width))
            cosine, sine = (
                jnp.dot(
                    packed[part], basis[part * slots : (part + 1) * slots, at],
                    preferred_element_type=jnp.float32,
                )
                for part in range(2)
            )
            parts = (
                cosine[:half] + sine[:half], cosine[half:] - sine[half:],
                cosine[half:] + sine[half:], cosine[:half] - sine[:half],
            )
            for j, x in enumerate(parts):
                quarters_ref[cycle, j * half : (j + 1) * half, at] = x.astype(quarters_ref.dtype)
        pltpu.make_async_copy(others, others, send_sem.at[cycle]).wait()


def basis_width():
    return -(-(NLON // 4 + 1) // LANES) * LANES


def cycle_quarters(points, cosine_sq, wave_of_slot, vorticity, divergence, legendre):
    slots, half, count = vorticity.shape
    lines = legendre.shape[1]
    cycles = points.shape[0]
    devices = lines // cycles
    columns = 4 * half
    rows = 6 * half
    width = basis_width()
    sb = slot_block(slots)
    blocks = slots // sb
    smem = pl.BlockSpec(memory_space=pltpu.SMEM)
    hbm = pl.BlockSpec(memory_space=pltpu.HBM)
    sem = pltpu.SemaphoreType.DMA((cycles,))
    return pl.pallas_call(
        functools.partial(exchange_kernel, send_groups(blocks)),
        in_specs=[smem] * 2 + [hbm] * 4,
        out_specs=pl.BlockSpec(memory_space=pltpu.VMEM),
        out_shape=jax.ShapeDtypeStruct((cycles, 2 * rows, width), jnp.bfloat16),
        scratch_shapes=[
            pltpu.VMEM(wave_of_slot.shape, jnp.int32),
            pltpu.VMEM((devices * slots, LANES), jnp.float32),
            pltpu.VMEM(vorticity.shape, vorticity.dtype),
            pltpu.VMEM(divergence.shape, divergence.dtype),
            pltpu.VMEM(legendre.shape, legendre.dtype),
            pltpu.VMEM((lines * sb, columns), jnp.float32),
            pltpu.VMEM((lines, blocks, sb, columns), jnp.bfloat16),
            pltpu.VMEM((cycles, devices, blocks, sb, columns), jnp.bfloat16),
            pltpu.VMEM((2 * devices * slots, width), jnp.bfloat16),
            pltpu.VMEM((2, rows, devices * slots), jnp.bfloat16),
            pltpu.SemaphoreType.DMA,
            pltpu.SemaphoreType.DMA((3, blocks)),
            sem,
            sem,
        ],
        compiler_params=pltpu.CompilerParams(
            collective_id=0, has_side_effects=True, vmem_limit_bytes=40 << 20
        ),
    )(points, cosine_sq, *(
        pltpu.with_memory_space_constraint(x, pltpu.HBM)
        for x in (wave_of_slot, vorticity, divergence, legendre)
    ))


def place(quarters, points, line):
    rows = quarters.shape[0] // 4
    width = quarters.shape[1]
    tiles = width // LANES
    quarter = points // 4
    lane = lax.broadcasted_iota(jnp.int32, (rows, LANES), 1)
    for j in range(4):
        turned = j % 2
        offset = quarter * (j + 1) - (width - 1) if turned else quarter * j
        offset = offset + front_lanes(width)
        base = pl.multiple_of(offset // LANES * LANES, LANES)
        shift = offset - base
        source = lane - shift if not turned else shift - 1 - lane
        source = source & (LANES - 1)
        previous = jnp.zeros((rows, LANES), jnp.float32)
        for t in range(tiles + 1):
            rolled = jnp.zeros((rows, LANES), jnp.float32)
            if t < tiles:
                u = tiles - 1 - t if turned else t
                tile = quarters[j * rows : (j + 1) * rows, u * LANES : (u + 1) * LANES]
                point = lane + u * LANES
                keep = (point > 0) & (point <= quarter) if turned else point < quarter
                tile = jnp.where(keep, tile.astype(jnp.float32), 0.0)
                rolled = jnp.take_along_axis(tile, source, axis=1)
            moved = jnp.where(lane < shift, previous, rolled).astype(line.dtype)
            at = pl.ds(pl.multiple_of(base + t * LANES, LANES), LANES)
            line[:, at] = line[:, at] + moved
            previous = rolled


def front_lanes(width):
    return width + LANES


def place_kernel(points_ref, quarters_ref, out_ref, line):
    line[...] = jnp.zeros_like(line)
    place(quarters_ref.at[0], points_ref[pl.program_id(0)], line)
    front = front_lanes(quarters_ref.shape[2])
    out_ref[0] = line[:, front : front + out_ref.shape[2]]


def placed(quarters, points):
    cycles, rows, width = quarters.shape
    rows = rows // 4
    line = front_lanes(width) + 4 * width + 2 * LANES
    return pl.pallas_call(
        place_kernel,
        grid=(cycles,),
        in_specs=[
            pl.BlockSpec(memory_space=pltpu.SMEM),
            pl.BlockSpec((1, 4 * rows, width), lambda i: (i, 0, 0)),
        ],
        out_specs=pl.BlockSpec((1, rows, NLON), lambda i: (i, 0, 0)),
        out_shape=jax.ShapeDtypeStruct((cycles, rows, NLON), jnp.bfloat16),
        scratch_shapes=[pltpu.VMEM((rows, line), jnp.bfloat16)],
        compiler_params=pltpu.CompilerParams(vmem_limit_bytes=16 << 20),
    )(points, quarters)


def body(vorticity, divergence, legendre, wave_of_slot, cycle_points, cos_squared):
    quarters = cycle_quarters(
        cycle_points, cos_squared, wave_of_slot, vorticity, divergence, legendre
    )
    return placed(quarters, cycle_points)


def solution(mesh):
    return jax.shard_map(
        body,
        mesh=mesh,
        in_specs=(
            P(("member", "wave"), None, None),
            P(("member", "wave"), None, None),
            P("wave", None, None),
            P(),
            P("wave"),
            P("wave"),
        ),
        out_specs=P(("member", "wave"), None, None),
        check_vma=False,
    )
```

```python
import functools

import jax
import jax.numpy as jnp
from jax import lax
from jax.experimental import pallas as pl
from jax.experimental.pallas import tpu as pltpu
from jax.sharding import PartitionSpec as P

NLON = 5136
LANES = 128
COS = (1.0, -1 / 2, 1 / 24, -1 / 720, 1 / 40320, -1 / 3628800, 1 / 479001600,
       -1 / 87178291200, 1 / 20922789888000, -1 / 6402373705728000)
SIN = (1.0, -1 / 6, 1 / 120, -1 / 5040, 1 / 362880, -1 / 39916800, 1 / 6227020800,
       -1 / 1307674368000, 1 / 355687428096000, -1 / 121645100408832000)


def slot_block(slots):
    return max(b for b in range(1, 17) if slots % b == 0)


def degree_coefs(wave, count):
    column = lax.broadcasted_iota(jnp.int32, (wave.shape[0], count), 1)
    degree = wave + column
    living = degree < count
    positive = living & (degree > 0)
    m = wave.astype(jnp.float32)
    n = degree.astype(jnp.float32)
    radius = count / 4.0
    square = n * n
    ratio = jnp.maximum(square - m * m, 0.0) / jnp.maximum(square * (4.0 * square - 1.0), 1.0)
    lower = radius * jnp.sqrt(ratio)
    upper = pltpu.roll(lower, count - 1, 1)
    along = jnp.where(positive, -radius * m / jnp.maximum(n * (n + 1.0), 1.0), 0.0)
    before = jnp.where(positive, -lower, 0.0)
    after = jnp.where((degree > 0) & (degree + 1 < count), upper, 0.0)
    return living.astype(jnp.float32), along, before, after


def slot_fourier(values, live, along, before, after, zd):
    count = values.shape[-1]
    p = values.astype(jnp.float32)
    lon = p * along
    up, down = pltpu.roll(values, 1, 1), pltpu.roll(values, count - 1, 1)
    lat = up.astype(jnp.float32) * before + down.astype(jnp.float32) * after
    left = jnp.concatenate([p * live, lon, lat], axis=0).astype(jnp.bfloat16)
    sums = lax.dot_general(left, zd, (((1,), (1,)), ((), ())), preferred_element_type=jnp.float32)
    rows = p.shape[0]
    lev = zd.shape[0] // 4
    plain, a, b = sums[:rows], sums[rows : 2 * rows], sums[2 * rows :]
    zr, zi, dr, di = (slice(g * lev, (g + 1) * lev) for g in range(4))
    turned = jnp.concatenate([-a[:, di], a[:, dr], -a[:, zi], a[:, zr]], axis=1)
    lane = lax.broadcasted_iota(jnp.int32, b.shape, 1)
    winds = turned + jnp.where(lane < 2 * lev, -b, b)
    return jnp.concatenate([winds, plain], axis=1)


def horner(coefs, x):
    total = jnp.full_like(x, coefs[-1])
    for c in coefs[-2::-1]:
        total = total * x + c
    return total


def turn(steps, points, per_point):
    turns = jnp.round(steps * per_point)
    theta = (steps - turns * points) * (per_point * (2.0 * jnp.pi))
    square = theta * theta
    return horner(COS, square), theta * horner(SIN, square)


def columns_of(row):
    return jnp.broadcast_to(row, (LANES, row.shape[1])).T


def fill_basis(wave_col, wave_row, points, basis):
    steps = turn(wave_row * float(LANES), points, 1.0 / points)
    step_c, step_s = (columns_of(x) for x in steps)
    slots = wave_col.shape[0]
    lane = lax.broadcasted_iota(jnp.int32, (16, LANES), 1).astype(jnp.float32)
    for start in range(0, slots, 16):
        rows = slice(start, start + 16)
        c, s = turn(wave_col[rows] * lane, points, 1.0 / points)
        cs, ss = step_c[rows], step_s[rows]
        for t in range(basis.shape[1] // LANES):
            at = slice(t * LANES, (t + 1) * LANES)
            basis[rows, at] = c.astype(basis.dtype)
            basis[slots + start : slots + start + 16, at] = s.astype(basis.dtype)
            c, s = c * cs - s * ss, s * cs + c * ss


def fill_fields(arrived, m, points, cosine_sq, count, packed, at):
    x = arrived.astype(jnp.float32).T
    lev = x.shape[0] // 8
    ur, ui, vr, vi, zr, zi, dr, di = (x[g * lev : (g + 1) * lev] for g in range(8))
    q = m * (4.0 / count)
    over = 1.0 / cosine_sq
    ulr, uli, vlr, vli = -q * ui, q * ur, -q * vi, q * vr
    fields = (
        (ur, ui), (vr, vi), (ulr, uli), (vlr, vli),
        (vlr * over - zr, vli * over - zi), (dr - ulr * over, di - uli * over),
    )
    weight = jnp.where(2.0 * m < points, jnp.where(m == 0.0, 1.0, 2.0), 0.0)
    parity = jnp.where((m.astype(jnp.int32) & 1) == 0, 1.0, -1.0)
    half = len(fields) * lev
    for f, (re, im) in enumerate(fields):
        for part, x in enumerate((re * weight, -im * weight)):
            packed[part, f * lev : (f + 1) * lev, at] = x.astype(packed.dtype)
            packed[part, half + f * lev : half + (f + 1) * lev, at] = (x * parity).astype(packed.dtype)


def in_halves(devices, blocks, sb):
    return devices % 2 == 0 and blocks > 1 and sb % 16 == 0


def partners(me, devices):
    if devices % 2:
        return [lax.rem(me + off, devices) for off in range(1, devices)], []
    half = devices // 2
    side = me // half
    far = [(1 - side) * half + lax.rem(me + off, half) for off in range(half)]
    near = [side * half + lax.rem(me + off, half) for off in range(1, half)]
    return far, near


def chunks_of(me, devices, blocks, sb):
    if not in_halves(devices, blocks, sb):
        return [(devices, 0, (0, blocks), 0, devices - 1)]
    half = devices // 2
    side = me // half
    other = 1 - side
    return [
        (half, side * half, (0, blocks), 0, half - 1),
        (half, other * half, (0, blocks - 1), 1, half),
        (half, other * half, (blocks - 1, blocks), 2, half),
    ]


def exchange_kernel(
    points_ref, cosine_ref, wave_hbm, zeta_hbm, delta_hbm, values_hbm, quarters_ref,
    wave_ref, wave_col, wave_order, zeta_ref, delta_ref, values_ref, sums, sent, held, basis, packed, total,
    wave_sem, in_sem, send_sem, recv_sem,
):
    cycles, devices, blocks, sb, columns = held.shape
    count = zeta_ref.shape[-1]
    rows = values_ref.shape[1]
    own = blocks * sb
    me = lax.axis_index("wave")
    barrier = pltpu.get_barrier_semaphore()
    far, near = partners(me, devices)
    halves = in_halves(devices, blocks, sb)
    pieces = 2 if sb % 2 == 0 else 1
    piece = sb // pieces

    def fetch(step, part):
        at = pl.ds(step * sb + part * piece, piece)
        return [
            pltpu.make_async_copy(source.at[at], target.at[at], in_sem.at[k, step, part])
            for k, (source, target) in enumerate(
                ((zeta_hbm, zeta_ref), (delta_hbm, delta_ref), (values_hbm, values_ref))
            )
        ]

    def start(step, part):
        for copy in fetch(step, part):
            copy.start()

    def start_step(step):
        for part in range(pieces):
            start(step, part)

    start(0, 0)
    load_wave = pltpu.make_async_copy(wave_hbm, wave_ref, wave_sem)
    load_wave.start()
    for to in far + near:
        pl.semaphore_signal(
            barrier, inc=1, device_id={"wave": to}, device_id_type=pl.DeviceIdType.MESH
        )
    for part in range(1, pieces):
        start(0, part)

    def send(step, last):
        for to, distant in [(to, True) for to in far] + [(to, False) for to in near]:
            slot = (2 if last else 1) if halves and distant else 0
            for cycle in range(cycles):
                pltpu.make_async_remote_copy(
                    src_ref=sent.at[to * cycles + cycle, step],
                    dst_ref=held.at[cycle, me, step],
                    send_sem=send_sem.at[cycle],
                    recv_sem=recv_sem.at[cycle, slot],
                    device_id={"wave": to},
                    device_id_type=pl.DeviceIdType.MESH,
                ).start()

    load_wave.wait()
    if blocks > 1:
        start_step(1)
    wave_col[...] = columns_of(wave_ref[...].reshape(1, -1).astype(jnp.float32))

    def coefs_of(step):
        waves = wave_col[pl.ds(me * own + step * sb, sb), 0:1].astype(jnp.int32)
        return degree_coefs(waves, count)

    def transform(step, coefs, slots):
        for s in slots:
            slot = step * sb + s
            zd = jnp.concatenate([zeta_ref[slot], delta_ref[slot]], axis=0)
            out = slot_fourier(values_ref[slot], *(c[s : s + 1] for c in coefs), zd)
            sums[pl.ds(s, rows, sb), :] = out

    def await_part(step, part):
        for copy in fetch(step, part):
            copy.wait()

    def legendre(step, first):
        if first:
            coefs = coefs_of(step)
            for part in range(pieces):
                await_part(step, part)
                if part == 0 and blocks > 2:
                    start_step(2)
                transform(step, coefs, range(part * piece, (part + 1) * piece))
        else:
            for part in range(pieces):
                await_part(step, part)
            pl.when(step + 2 < blocks)(lambda: start_step(step + 2))
            transform(step, coefs_of(step), range(sb))
        sent[:, step] = sums[...].astype(sent.dtype).reshape(rows, sb, columns)
        for cycle in range(cycles):
            mine = sums[pl.ds((me * cycles + cycle) * sb, sb), :]
            held[cycle, me, step] = mine.astype(held.dtype)

    legendre(0, True)
    pl.semaphore_wait(barrier, devices - 1)
    send(0, blocks == 1)

    def middle(step, carry):
        legendre(step, False)
        pl.when(step < blocks - 1)(lambda: send(step, False))
        pl.when(step == blocks - 1)(lambda: send(step, True))
        return carry

    lax.fori_loop(1, blocks, middle, 0)
    chunks = chunks_of(me, devices, blocks, sb)
    spans = []
    for sources, first, (low, high), _, _ in chunks:
        at = spans[-1].stop if spans else 0
        spans.append(slice(at, at + sources * (high - low) * sb))
        if high - low == blocks:
            wave_order[spans[-1]] = wave_col[pl.ds(first * own, sources * own)]
        else:
            for r in range(sources):
                size = (high - low) * sb
                wave_order[at + r * size : at + (r + 1) * size] = wave_col[
                    pl.ds((first + r) * own + low * sb, size)
                ]
    slots = wave_order.shape[0]
    wave_row = wave_order[...].T[0:1]
    for cycle in range(cycles):
        points = jnp.full((1, 1), points_ref[cycle], jnp.int32).astype(jnp.float32)
        cosine_sq = jnp.full((1, 1), cosine_ref[cycle], jnp.float32)
        fill_basis(wave_order, wave_row, points, basis)
        width = basis.shape[1]
        half = packed.shape[1] // 2
        for number, (sources, first, (low, high), slot, copies) in enumerate(chunks):
            span = spans[number]
            arriving = held.at[cycle, 0:copies, low:high]
            pltpu.make_async_copy(arriving, arriving, recv_sem.at[cycle, slot]).wait()
            arrived = held[cycle, pl.ds(first, sources), low:high].reshape(-1, columns)
            fill_fields(arrived, wave_row[:, span], points, cosine_sq, count, packed, span)
            for begin in range(0, width, 256):
                at = slice(begin, min(begin + 256, width))
                both = []
                for part in range(2):
                    x = jnp.dot(
                        packed[part, :, span],
                        basis[part * slots + span.start : part * slots + span.stop, at],
                        preferred_element_type=jnp.float32,
                    )
                    if number > 0:
                        x = total[part, :, at] + x
                    if number < len(chunks) - 1:
                        total[part, :, at] = x
                    both.append(x)
                if number == len(chunks) - 1:
                    cosine, sine = both
                    parts = (
                        cosine[:half] + sine[:half], cosine[half:] - sine[half:],
                        cosine[half:] + sine[half:], cosine[:half] - sine[:half],
                    )
                    for j, x in enumerate(parts):
                        quarters_ref[cycle, j * half : (j + 1) * half, at] = x.astype(quarters_ref.dtype)
    for cycle in range(cycles):
        others = held.at[cycle, 0 : devices - 1]
        pltpu.make_async_copy(others, others, send_sem.at[cycle]).wait()


def basis_width():
    return -(-(NLON // 4 + 1) // LANES) * LANES


def cycle_quarters(points, cosine_sq, wave_of_slot, vorticity, divergence, legendre):
    slots, half, count = vorticity.shape
    lines = legendre.shape[1]
    cycles = points.shape[0]
    devices = lines // cycles
    columns = 4 * half
    rows = 6 * half
    width = basis_width()
    sb = slot_block(slots)
    blocks = slots // sb
    hbm = pl.BlockSpec(memory_space=pltpu.HBM)
    return pl.pallas_call(
        exchange_kernel,
        in_specs=[pl.BlockSpec(memory_space=pltpu.SMEM)] * 2 + [hbm] * 4,
        out_specs=pl.BlockSpec(memory_space=pltpu.VMEM),
        out_shape=jax.ShapeDtypeStruct((cycles, 2 * rows, width), jnp.bfloat16),
        scratch_shapes=[
            pltpu.VMEM(wave_of_slot.shape, jnp.int32),
            pltpu.VMEM((devices * slots, LANES), jnp.float32),
            pltpu.VMEM((devices * slots, LANES), jnp.float32),
            pltpu.VMEM(vorticity.shape, vorticity.dtype),
            pltpu.VMEM(divergence.shape, divergence.dtype),
            pltpu.VMEM(legendre.shape, legendre.dtype),
            pltpu.VMEM((lines * sb, columns), jnp.float32),
            pltpu.VMEM((lines, blocks, sb, columns), jnp.bfloat16),
            pltpu.VMEM((cycles, devices, blocks, sb, columns), jnp.bfloat16),
            pltpu.VMEM((2 * devices * slots, width), jnp.bfloat16),
            pltpu.VMEM((2, rows, devices * slots), jnp.bfloat16),
            pltpu.VMEM((2, rows, width), jnp.float32),
            pltpu.SemaphoreType.DMA,
            pltpu.SemaphoreType.DMA((3, blocks, 2)),
            pltpu.SemaphoreType.DMA((cycles,)),
            pltpu.SemaphoreType.DMA((cycles, 3)),
        ],
        compiler_params=pltpu.CompilerParams(
            collective_id=0, has_side_effects=True, vmem_limit_bytes=44 << 20
        ),
    )(points, cosine_sq, *(
        pltpu.with_memory_space_constraint(x, pltpu.HBM)
        for x in (wave_of_slot, vorticity, divergence, legendre)
    ))


def place(quarters, first, points, line):
    rows = line.shape[0]
    width = quarters.shape[1]
    field = quarters.shape[0] // 4
    tiles = width // LANES
    quarter = points // 4
    lane = lax.broadcasted_iota(jnp.int32, (rows, LANES), 1)
    for j in range(4):
        turned = j % 2
        offset = quarter * (j + 1) - (width - 1) if turned else quarter * j
        offset = offset + front_lanes(width)
        base = pl.multiple_of(offset // LANES * LANES, LANES)
        shift = offset - base
        source = lane - shift if not turned else shift - 1 - lane
        source = source & (LANES - 1)
        previous = jnp.zeros((rows, LANES), jnp.float32)
        for t in range(tiles + 1):
            rolled = jnp.zeros((rows, LANES), jnp.float32)
            if t < tiles:
                u = tiles - 1 - t if turned else t
                tile = quarters[pl.ds(first + j * field, rows), u * LANES : (u + 1) * LANES]
                point = lane + u * LANES
                keep = (point > 0) & (point <= quarter) if turned else point < quarter
                tile = jnp.where(keep, tile.astype(jnp.float32), 0.0)
                rolled = jnp.take_along_axis(tile, source, axis=1)
            moved = jnp.where(lane < shift, previous, rolled).astype(line.dtype)
            at = pl.ds(pl.multiple_of(base + t * LANES, LANES), LANES)
            line[:, at] = line[:, at] + moved
            previous = rolled


def front_lanes(width):
    return width + LANES


def place_kernel(points_ref, quarters_ref, out_ref, line):
    cycle = pl.program_id(0)
    points = points_ref[cycle]
    line[...] = jnp.zeros_like(line)
    first = pl.multiple_of(pl.program_id(1) * line.shape[0], line.shape[0])
    place(quarters_ref.at[cycle], first, points, line)
    front = front_lanes(quarters_ref.shape[2])
    out_ref[0] = line[:, front : front + out_ref.shape[2]]


def row_block(rows):
    return rows


def placed(quarters, points):
    cycles, rows, width = quarters.shape
    rows = rows // 4
    step = row_block(rows)
    line = front_lanes(width) + 4 * width + 2 * LANES
    vmem = pl.BlockSpec(memory_space=pltpu.VMEM)
    return pl.pallas_call(
        place_kernel,
        grid=(cycles, rows // step),
        in_specs=[pl.BlockSpec(memory_space=pltpu.SMEM), vmem],
        out_specs=pl.BlockSpec((1, step, NLON), lambda i, k: (i, k, 0)),
        out_shape=jax.ShapeDtypeStruct((cycles, rows, NLON), jnp.bfloat16),
        scratch_shapes=[pltpu.VMEM((step, line), jnp.bfloat16)],
        compiler_params=pltpu.CompilerParams(vmem_limit_bytes=16 << 20),
    )(points, quarters)


def body(vorticity, divergence, legendre, wave_of_slot, cycle_points, cos_squared):
    quarters = cycle_quarters(
        cycle_points, cos_squared, wave_of_slot, vorticity, divergence, legendre
    )
    return placed(quarters, cycle_points)


def solution(mesh):
    return jax.shard_map(
        body,
        mesh=mesh,
        in_specs=(
            P(("member", "wave"), None, None),
            P(("member", "wave"), None, None),
            P("wave", None, None),
            P(),
            P("wave"),
            P("wave"),
        ),
        out_specs=P(("member", "wave"), None, None),
        check_vma=False,
    )
```

```python
import functools

import jax
import jax.numpy as jnp
from jax import lax
from jax.experimental import pallas as pl
from jax.experimental.pallas import tpu as pltpu
from jax.sharding import PartitionSpec as P

NLON = 5136
LANES = 128
COS = (1.0, -1 / 2, 1 / 24, -1 / 720, 1 / 40320, -1 / 3628800, 1 / 479001600,
       -1 / 87178291200, 1 / 20922789888000, -1 / 6402373705728000)
SIN = (1.0, -1 / 6, 1 / 120, -1 / 5040, 1 / 362880, -1 / 39916800, 1 / 6227020800,
       -1 / 1307674368000, 1 / 355687428096000, -1 / 121645100408832000)


def slot_block(slots):
    return max(b for b in range(1, 17) if slots % b == 0)


def degree_coefs(wave, count):
    column = lax.broadcasted_iota(jnp.int32, (wave.shape[0], count), 1)
    degree = wave + column
    living = degree < count
    positive = living & (degree > 0)
    m = wave.astype(jnp.float32)
    n = degree.astype(jnp.float32)
    radius = count / 4.0
    square = n * n
    ratio = jnp.maximum(square - m * m, 0.0) / jnp.maximum(square * (4.0 * square - 1.0), 1.0)
    lower = radius * jnp.sqrt(ratio)
    upper = pltpu.roll(lower, count - 1, 1)
    along = jnp.where(positive, -radius * m / jnp.maximum(n * (n + 1.0), 1.0), 0.0)
    before = jnp.where(positive, -lower, 0.0)
    after = jnp.where((degree > 0) & (degree + 1 < count), upper, 0.0)
    return living.astype(jnp.float32), along, before, after


def slot_fourier(values, live, along, before, after, zd):
    count = values.shape[-1]
    p = values.astype(jnp.float32)
    lon = p * along
    up, down = pltpu.roll(values, 1, 1), pltpu.roll(values, count - 1, 1)
    lat = up.astype(jnp.float32) * before + down.astype(jnp.float32) * after
    left = jnp.concatenate([p * live, lon, lat], axis=0).astype(jnp.bfloat16)
    sums = lax.dot_general(left, zd, (((1,), (1,)), ((), ())), preferred_element_type=jnp.float32)
    rows = p.shape[0]
    lev = zd.shape[0] // 4
    plain, a, b = sums[:rows], sums[rows : 2 * rows], sums[2 * rows :]
    zr, zi, dr, di = (slice(g * lev, (g + 1) * lev) for g in range(4))
    turned = jnp.concatenate([-a[:, di], a[:, dr], -a[:, zi], a[:, zr]], axis=1)
    lane = lax.broadcasted_iota(jnp.int32, b.shape, 1)
    winds = turned + jnp.where(lane < 2 * lev, -b, b)
    return jnp.concatenate([winds, plain], axis=1)


def horner(coefs, x):
    total = jnp.full_like(x, coefs[-1])
    for c in coefs[-2::-1]:
        total = total * x + c
    return total


def turn(steps, points, per_point):
    turns = jnp.round(steps * per_point)
    theta = (steps - turns * points) * (per_point * (2.0 * jnp.pi))
    square = theta * theta
    return horner(COS, square), theta * horner(SIN, square)


def columns_of(row):
    return jnp.broadcast_to(row, (LANES, row.shape[1])).T


def fill_basis(wave_col, wave_row, points, basis):
    steps = turn(wave_row * float(LANES), points, 1.0 / points)
    step_c, step_s = (columns_of(x) for x in steps)
    slots = wave_col.shape[0]
    lane = lax.broadcasted_iota(jnp.int32, (16, LANES), 1).astype(jnp.float32)
    for start in range(0, slots, 16):
        rows = slice(start, start + 16)
        c, s = turn(wave_col[rows] * lane, points, 1.0 / points)
        cs, ss = step_c[rows], step_s[rows]
        for t in range(basis.shape[1] // LANES):
            at = slice(t * LANES, (t + 1) * LANES)
            basis[rows, at] = c.astype(basis.dtype)
            basis[slots + start : slots + start + 16, at] = s.astype(basis.dtype)
            c, s = c * cs - s * ss, s * cs + c * ss


def fill_fields(arrived, m, points, cosine_sq, count, packed, at):
    x = arrived.astype(jnp.float32).T
    lev = x.shape[0] // 8
    ur, ui, vr, vi, zr, zi, dr, di = (x[g * lev : (g + 1) * lev] for g in range(8))
    q = m * (4.0 / count)
    over = 1.0 / cosine_sq
    ulr, uli, vlr, vli = -q * ui, q * ur, -q * vi, q * vr
    fields = (
        (ur, ui), (vr, vi), (ulr, uli), (vlr, vli),
        (vlr * over - zr, vli * over - zi), (dr - ulr * over, di - uli * over),
    )
    weight = jnp.where(2.0 * m < points, jnp.where(m == 0.0, 1.0, 2.0), 0.0)
    parity = jnp.where((m.astype(jnp.int32) & 1) == 0, 1.0, -1.0)
    half = len(fields) * lev
    for f, (re, im) in enumerate(fields):
        for part, x in enumerate((re * weight, -im * weight)):
            packed[part, f * lev : (f + 1) * lev, at] = x.astype(packed.dtype)
            packed[part, half + f * lev : half + (f + 1) * lev, at] = (x * parity).astype(packed.dtype)


def in_halves(devices, blocks, sb):
    return devices % 2 == 0 and blocks > 1 and sb % 16 == 0


def partners(me, devices):
    if devices % 2:
        return [lax.rem(me + off, devices) for off in range(1, devices)], []
    half = devices // 2
    side = me // half
    run = half // 2 if half % 2 == 0 else half
    far = []
    for turn_of in range(half // run):
        base = side * (turn_of * run) + (1 - side) * (devices - (turn_of + 1) * run)
        far += [base + lax.rem(me + off, run) for off in range(run)]
    near = [side * half + lax.rem(me + off, half) for off in range(1, half)]
    return far, near


def chunks_of(me, devices, blocks, sb):
    if not in_halves(devices, blocks, sb):
        return [(devices, 0, (0, blocks), 0, devices - 1)]
    half = devices // 2
    side = me // half
    other = 1 - side
    return [
        (half, side * half, (0, blocks), 0, half - 1),
        (half, other * half, (0, blocks - 1), 1, half),
        (half, other * half, (blocks - 1, blocks), 2, half),
    ]


def exchange_kernel(
    points_ref, cosine_ref, wave_hbm, zeta_hbm, delta_hbm, values_hbm, quarters_ref,
    wave_ref, wave_col, wave_order, zeta_ref, delta_ref, values_ref, sums, sent, held, basis, packed, total,
    wave_sem, in_sem, send_sem, recv_sem,
):
    cycles, devices, blocks, sb, columns = held.shape
    count = zeta_ref.shape[-1]
    rows = values_ref.shape[1]
    own = blocks * sb
    me = lax.axis_index("wave")
    barrier = pltpu.get_barrier_semaphore()
    far, near = partners(me, devices)
    halves = in_halves(devices, blocks, sb)
    pieces = 2 if sb % 2 == 0 else 1
    piece = sb // pieces

    def fetch(step, part):
        at = pl.ds(step * sb + part * piece, piece)
        return [
            pltpu.make_async_copy(source.at[at], target.at[at], in_sem.at[k, step, part])
            for k, (source, target) in enumerate(
                ((zeta_hbm, zeta_ref), (delta_hbm, delta_ref), (values_hbm, values_ref))
            )
        ]

    def start(step, part):
        for copy in fetch(step, part):
            copy.start()

    def start_step(step):
        for part in range(pieces):
            start(step, part)

    start(0, 0)
    load_wave = pltpu.make_async_copy(wave_hbm, wave_ref, wave_sem)
    load_wave.start()
    for to in far + near:
        pl.semaphore_signal(
            barrier, inc=1, device_id={"wave": to}, device_id_type=pl.DeviceIdType.MESH
        )
    for part in range(1, pieces):
        start(0, part)

    def send(step, last):
        for to, distant in [(to, True) for to in far] + [(to, False) for to in near]:
            slot = (2 if last else 1) if halves and distant else 0
            for cycle in range(cycles):
                pltpu.make_async_remote_copy(
                    src_ref=sent.at[to * cycles + cycle, step],
                    dst_ref=held.at[cycle, me, step],
                    send_sem=send_sem.at[cycle],
                    recv_sem=recv_sem.at[cycle, slot],
                    device_id={"wave": to},
                    device_id_type=pl.DeviceIdType.MESH,
                ).start()

    load_wave.wait()
    if blocks > 1:
        start_step(1)
    wave_col[...] = columns_of(wave_ref[...].reshape(1, -1).astype(jnp.float32))

    def coefs_of(step):
        waves = wave_col[pl.ds(me * own + step * sb, sb), 0:1].astype(jnp.int32)
        return degree_coefs(waves, count)

    def transform(step, coefs, slots):
        for s in slots:
            slot = step * sb + s
            zd = jnp.concatenate([zeta_ref[slot], delta_ref[slot]], axis=0)
            out = slot_fourier(values_ref[slot], *(c[s : s + 1] for c in coefs), zd)
            sums[pl.ds(s, rows, sb), :] = out

    def await_part(step, part):
        for copy in fetch(step, part):
            copy.wait()

    def legendre(step, first):
        if first:
            coefs = coefs_of(step)
            for part in range(pieces):
                await_part(step, part)
                if part == 0 and blocks > 2:
                    start_step(2)
                transform(step, coefs, range(part * piece, (part + 1) * piece))
        else:
            for part in range(pieces):
                await_part(step, part)
            pl.when(step + 2 < blocks)(lambda: start_step(step + 2))
            transform(step, coefs_of(step), range(sb))
        sent[:, step] = sums[...].astype(sent.dtype).reshape(rows, sb, columns)
        for cycle in range(cycles):
            mine = sums[pl.ds((me * cycles + cycle) * sb, sb), :]
            held[cycle, me, step] = mine.astype(held.dtype)

    legendre(0, True)
    pl.semaphore_wait(barrier, devices - 1)
    send(0, blocks == 1)

    def middle(step, carry):
        legendre(step, False)
        pl.when(step < blocks - 1)(lambda: send(step, False))
        pl.when(step == blocks - 1)(lambda: send(step, True))
        return carry

    lax.fori_loop(1, blocks, middle, 0)
    chunks = chunks_of(me, devices, blocks, sb)
    spans = []
    for sources, first, (low, high), _, _ in chunks:
        at = spans[-1].stop if spans else 0
        spans.append(slice(at, at + sources * (high - low) * sb))
        if high - low == blocks:
            wave_order[spans[-1]] = wave_col[pl.ds(first * own, sources * own)]
        else:
            for r in range(sources):
                size = (high - low) * sb
                wave_order[at + r * size : at + (r + 1) * size] = wave_col[
                    pl.ds((first + r) * own + low * sb, size)
                ]
    slots = wave_order.shape[0]
    wave_row = wave_order[...].T[0:1]
    for cycle in range(cycles):
        points = jnp.full((1, 1), points_ref[cycle], jnp.int32).astype(jnp.float32)
        cosine_sq = jnp.full((1, 1), cosine_ref[cycle], jnp.float32)
        fill_basis(wave_order, wave_row, points, basis)
        width = basis.shape[1]
        half = packed.shape[1] // 2
        for number, (sources, first, (low, high), slot, copies) in enumerate(chunks):
            span = spans[number]
            arriving = held.at[cycle, 0:copies, low:high]
            pltpu.make_async_copy(arriving, arriving, recv_sem.at[cycle, slot]).wait()
            arrived = held[cycle, pl.ds(first, sources), low:high].reshape(-1, columns)
            fill_fields(arrived, wave_row[:, span], points, cosine_sq, count, packed, span)
            for begin in range(0, width, 256):
                at = slice(begin, min(begin + 256, width))
                both = []
                for part in range(2):
                    x = jnp.dot(
                        packed[part, :, span],
                        basis[part * slots + span.start : part * slots + span.stop, at],
                        preferred_element_type=jnp.float32,
                    )
                    if number > 0:
                        x = total[part, :, at] + x
                    if number < len(chunks) - 1:
                        total[part, :, at] = x
                    both.append(x)
                if number == len(chunks) - 1:
                    cosine, sine = both
                    parts = (
                        cosine[:half] + sine[:half], cosine[half:] - sine[half:],
                        cosine[half:] + sine[half:], cosine[:half] - sine[:half],
                    )
                    for j, x in enumerate(parts):
                        quarters_ref[cycle, j * half : (j + 1) * half, at] = x.astype(quarters_ref.dtype)
    for cycle in range(cycles):
        others = held.at[cycle, 0 : devices - 1]
        pltpu.make_async_copy(others, others, send_sem.at[cycle]).wait()


def basis_width():
    return -(-(NLON // 4 + 1) // LANES) * LANES


def cycle_quarters(points, cosine_sq, wave_of_slot, vorticity, divergence, legendre):
    slots, half, count = vorticity.shape
    lines = legendre.shape[1]
    cycles = points.shape[0]
    devices = lines // cycles
    columns = 4 * half
    rows = 6 * half
    width = basis_width()
    sb = slot_block(slots)
    blocks = slots // sb
    hbm = pl.BlockSpec(memory_space=pltpu.HBM)
    return pl.pallas_call(
        exchange_kernel,
        in_specs=[pl.BlockSpec(memory_space=pltpu.SMEM)] * 2 + [hbm] * 4,
        out_specs=pl.BlockSpec(memory_space=pltpu.VMEM),
        out_shape=jax.ShapeDtypeStruct((cycles, 2 * rows, width), jnp.bfloat16),
        scratch_shapes=[
            pltpu.VMEM(wave_of_slot.shape, jnp.int32),
            pltpu.VMEM((devices * slots, LANES), jnp.float32),
            pltpu.VMEM((devices * slots, LANES), jnp.float32),
            pltpu.VMEM(vorticity.shape, vorticity.dtype),
            pltpu.VMEM(divergence.shape, divergence.dtype),
            pltpu.VMEM(legendre.shape, legendre.dtype),
            pltpu.VMEM((lines * sb, columns), jnp.float32),
            pltpu.VMEM((lines, blocks, sb, columns), jnp.bfloat16),
            pltpu.VMEM((cycles, devices, blocks, sb, columns), jnp.bfloat16),
            pltpu.VMEM((2 * devices * slots, width), jnp.bfloat16),
            pltpu.VMEM((2, rows, devices * slots), jnp.bfloat16),
            pltpu.VMEM((2, rows, width), jnp.float32),
            pltpu.SemaphoreType.DMA,
            pltpu.SemaphoreType.DMA((3, blocks, 2)),
            pltpu.SemaphoreType.DMA((cycles,)),
            pltpu.SemaphoreType.DMA((cycles, 3)),
        ],
        compiler_params=pltpu.CompilerParams(
            collective_id=0, has_side_effects=True, vmem_limit_bytes=44 << 20
        ),
    )(points, cosine_sq, *(
        pltpu.with_memory_space_constraint(x, pltpu.HBM)
        for x in (wave_of_slot, vorticity, divergence, legendre)
    ))


def place(quarters, first, points, line):
    rows = line.shape[0]
    width = quarters.shape[1]
    field = quarters.shape[0] // 4
    tiles = width // LANES
    quarter = points // 4
    lane = lax.broadcasted_iota(jnp.int32, (rows, LANES), 1)
    for j in range(4):
        turned = j % 2
        offset = quarter * (j + 1) - (width - 1) if turned else quarter * j
        offset = offset + front_lanes(width)
        base = pl.multiple_of(offset // LANES * LANES, LANES)
        shift = offset - base
        source = lane - shift if not turned else shift - 1 - lane
        source = source & (LANES - 1)
        previous = jnp.zeros((rows, LANES), jnp.float32)
        for t in range(tiles + 1):
            rolled = jnp.zeros((rows, LANES), jnp.float32)
            if t < tiles:
                u = tiles - 1 - t if turned else t
                tile = quarters[pl.ds(first + j * field, rows), u * LANES : (u + 1) * LANES]
                point = lane + u * LANES
                keep = (point > 0) & (point <= quarter) if turned else point < quarter
                tile = jnp.where(keep, tile.astype(jnp.float32), 0.0)
                rolled = jnp.take_along_axis(tile, source, axis=1)
            moved = jnp.where(lane < shift, previous, rolled).astype(line.dtype)
            at = pl.ds(pl.multiple_of(base + t * LANES, LANES), LANES)
            line[:, at] = line[:, at] + moved
            previous = rolled


def front_lanes(width):
    return width + LANES


def place_kernel(points_ref, quarters_ref, out_ref, line):
    cycle = pl.program_id(0)
    points = points_ref[cycle]
    line[...] = jnp.zeros_like(line)
    first = pl.multiple_of(pl.program_id(1) * line.shape[0], line.shape[0])
    place(quarters_ref.at[cycle], first, points, line)
    front = front_lanes(quarters_ref.shape[2])
    out_ref[0] = line[:, front : front + out_ref.shape[2]]


def row_block(rows):
    return rows


def placed(quarters, points):
    cycles, rows, width = quarters.shape
    rows = rows // 4
    step = row_block(rows)
    line = front_lanes(width) + 4 * width + 2 * LANES
    vmem = pl.BlockSpec(memory_space=pltpu.VMEM)
    return pl.pallas_call(
        place_kernel,
        grid=(cycles, rows // step),
        in_specs=[pl.BlockSpec(memory_space=pltpu.SMEM), vmem],
        out_specs=pl.BlockSpec((1, step, NLON), lambda i, k: (i, k, 0)),
        out_shape=jax.ShapeDtypeStruct((cycles, rows, NLON), jnp.bfloat16),
        scratch_shapes=[pltpu.VMEM((step, line), jnp.bfloat16)],
        compiler_params=pltpu.CompilerParams(vmem_limit_bytes=16 << 20),
    )(points, quarters)


def body(vorticity, divergence, legendre, wave_of_slot, cycle_points, cos_squared):
    quarters = cycle_quarters(
        cycle_points, cos_squared, wave_of_slot, vorticity, divergence, legendre
    )
    return placed(quarters, cycle_points)


def solution(mesh):
    return jax.shard_map(
        body,
        mesh=mesh,
        in_specs=(
            P(("member", "wave"), None, None),
            P(("member", "wave"), None, None),
            P("wave", None, None),
            P(),
            P("wave"),
            P("wave"),
        ),
        out_specs=P(("member", "wave"), None, None),
        check_vma=False,
    )
```

```python
import functools

import jax
import jax.numpy as jnp
from jax import lax
from jax.experimental import pallas as pl
from jax.experimental.pallas import tpu as pltpu
from jax.sharding import PartitionSpec as P

NLON = 5136
LANES = 128
COS = (1.0, -1 / 2, 1 / 24, -1 / 720, 1 / 40320, -1 / 3628800, 1 / 479001600,
       -1 / 87178291200, 1 / 20922789888000, -1 / 6402373705728000)
SIN = (1.0, -1 / 6, 1 / 120, -1 / 5040, 1 / 362880, -1 / 39916800, 1 / 6227020800,
       -1 / 1307674368000, 1 / 355687428096000, -1 / 121645100408832000)


def slot_block(slots):
    return max(b for b in range(1, 17) if slots % b == 0)


def degree_coefs(wave, count):
    column = lax.broadcasted_iota(jnp.int32, (wave.shape[0], count), 1)
    degree = wave + column
    living = degree < count
    positive = living & (degree > 0)
    m = wave.astype(jnp.float32)
    n = degree.astype(jnp.float32)
    radius = count / 4.0
    square = n * n
    ratio = jnp.maximum(square - m * m, 0.0) / jnp.maximum(square * (4.0 * square - 1.0), 1.0)
    lower = radius * jnp.sqrt(ratio)
    upper = pltpu.roll(lower, count - 1, 1)
    along = jnp.where(positive, -radius * m / jnp.maximum(n * (n + 1.0), 1.0), 0.0)
    before = jnp.where(positive, -lower, 0.0)
    after = jnp.where((degree > 0) & (degree + 1 < count), upper, 0.0)
    return living.astype(jnp.float32), along, before, after


def slot_fourier(values, live, along, before, after, zd):
    count = values.shape[-1]
    p = values.astype(jnp.float32)
    lon = p * along
    up, down = pltpu.roll(values, 1, 1), pltpu.roll(values, count - 1, 1)
    lat = up.astype(jnp.float32) * before + down.astype(jnp.float32) * after
    left = jnp.concatenate([p * live, lon, lat], axis=0).astype(jnp.bfloat16)
    sums = lax.dot_general(left, zd, (((1,), (1,)), ((), ())), preferred_element_type=jnp.float32)
    rows = p.shape[0]
    lev = zd.shape[0] // 4
    plain, a, b = sums[:rows], sums[rows : 2 * rows], sums[2 * rows :]
    zr, zi, dr, di = (slice(g * lev, (g + 1) * lev) for g in range(4))
    turned = jnp.concatenate([-a[:, di], a[:, dr], -a[:, zi], a[:, zr]], axis=1)
    lane = lax.broadcasted_iota(jnp.int32, b.shape, 1)
    winds = turned + jnp.where(lane < 2 * lev, -b, b)
    return jnp.concatenate([winds, plain], axis=1)


def horner(coefs, x):
    total = jnp.full_like(x, coefs[-1])
    for c in coefs[-2::-1]:
        total = total * x + c
    return total


def turn(steps, points, per_point):
    turns = jnp.round(steps * per_point)
    theta = (steps - turns * points) * (per_point * (2.0 * jnp.pi))
    square = theta * theta
    return horner(COS, square), theta * horner(SIN, square)


def columns_of(row):
    return jnp.broadcast_to(row, (LANES, row.shape[1])).T


def fill_basis(wave_col, wave_row, points, basis):
    steps = turn(wave_row * float(LANES), points, 1.0 / points)
    step_c, step_s = (columns_of(x) for x in steps)
    slots = wave_col.shape[0]
    lane = lax.broadcasted_iota(jnp.int32, (16, LANES), 1).astype(jnp.float32)
    for start in range(0, slots, 16):
        rows = slice(start, start + 16)
        c, s = turn(wave_col[rows] * lane, points, 1.0 / points)
        cs, ss = step_c[rows], step_s[rows]
        for t in range(basis.shape[1] // LANES):
            at = slice(t * LANES, (t + 1) * LANES)
            basis[rows, at] = c.astype(basis.dtype)
            basis[slots + start : slots + start + 16, at] = s.astype(basis.dtype)
            c, s = c * cs - s * ss, s * cs + c * ss


def fill_fields(arrived, m, points, cosine_sq, count, packed, at):
    x = arrived.astype(jnp.float32).T
    lev = x.shape[0] // 8
    ur, ui, vr, vi, zr, zi, dr, di = (x[g * lev : (g + 1) * lev] for g in range(8))
    q = m * (4.0 / count)
    over = 1.0 / cosine_sq
    ulr, uli, vlr, vli = -q * ui, q * ur, -q * vi, q * vr
    fields = (
        (ur, ui), (vr, vi), (ulr, uli), (vlr, vli),
        (vlr * over - zr, vli * over - zi), (dr - ulr * over, di - uli * over),
    )
    weight = jnp.where(2.0 * m < points, jnp.where(m == 0.0, 1.0, 2.0), 0.0)
    parity = jnp.where((m.astype(jnp.int32) & 1) == 0, 1.0, -1.0)
    half = len(fields) * lev
    for f, (re, im) in enumerate(fields):
        for part, x in enumerate((re * weight, -im * weight)):
            packed[part, f * lev : (f + 1) * lev, at] = x.astype(packed.dtype)
            packed[part, half + f * lev : half + (f + 1) * lev, at] = (x * parity).astype(packed.dtype)


def in_halves(devices, blocks, sb):
    return devices % 2 == 0 and blocks > 1 and sb % 16 == 0


def partners(me, devices):
    if devices % 2:
        return [lax.rem(me + off, devices) for off in range(1, devices)], []
    half = devices // 2
    side = me // half
    run = half // 2 if half % 2 == 0 else half
    far = []
    for turn_of in range(half // run):
        base = side * (turn_of * run) + (1 - side) * (devices - (turn_of + 1) * run)
        far += [base + side * off + (1 - side) * (run - 1 - off) for off in range(run)]
    near = [side * half + lax.rem(me + off, half) for off in range(1, half)]
    return far, near


def chunks_of(me, devices, blocks, sb):
    if not in_halves(devices, blocks, sb):
        return [(devices, 0, (0, blocks), 0, devices - 1)]
    half = devices // 2
    side = me // half
    other = 1 - side
    return [
        (half, side * half, (0, blocks), 0, half - 1),
        (half, other * half, (0, blocks - 1), 1, half),
        (half, other * half, (blocks - 1, blocks), 2, half),
    ]


def exchange_kernel(
    points_ref, cosine_ref, wave_hbm, zeta_hbm, delta_hbm, values_hbm, quarters_ref,
    wave_ref, wave_col, wave_order, zeta_ref, delta_ref, values_ref, sums, sent, held, basis, packed, total,
    wave_sem, in_sem, send_sem, recv_sem,
):
    cycles, devices, blocks, sb, columns = held.shape
    count = zeta_ref.shape[-1]
    rows = values_ref.shape[1]
    own = blocks * sb
    me = lax.axis_index("wave")
    barrier = pltpu.get_barrier_semaphore()
    far, near = partners(me, devices)
    halves = in_halves(devices, blocks, sb)
    pieces = 2 if sb % 2 == 0 else 1
    piece = sb // pieces

    def fetch(step, part):
        at = pl.ds(step * sb + part * piece, piece)
        return [
            pltpu.make_async_copy(source.at[at], target.at[at], in_sem.at[k, step, part])
            for k, (source, target) in enumerate(
                ((zeta_hbm, zeta_ref), (delta_hbm, delta_ref), (values_hbm, values_ref))
            )
        ]

    def start(step, part):
        for copy in fetch(step, part):
            copy.start()

    def start_step(step):
        for part in range(pieces):
            start(step, part)

    start(0, 0)
    load_wave = pltpu.make_async_copy(wave_hbm, wave_ref, wave_sem)
    load_wave.start()
    for to in far + near:
        pl.semaphore_signal(
            barrier, inc=1, device_id={"wave": to}, device_id_type=pl.DeviceIdType.MESH
        )
    for part in range(1, pieces):
        start(0, part)

    def send(step, last):
        for to, distant in [(to, True) for to in far] + [(to, False) for to in near]:
            slot = (2 if last else 1) if halves and distant else 0
            for cycle in range(cycles):
                pltpu.make_async_remote_copy(
                    src_ref=sent.at[to * cycles + cycle, step],
                    dst_ref=held.at[cycle, me, step],
                    send_sem=send_sem.at[cycle],
                    recv_sem=recv_sem.at[cycle, slot],
                    device_id={"wave": to},
                    device_id_type=pl.DeviceIdType.MESH,
                ).start()

    load_wave.wait()
    if blocks > 1:
        start_step(1)
    wave_col[...] = columns_of(wave_ref[...].reshape(1, -1).astype(jnp.float32))

    def coefs_of(step):
        waves = wave_col[pl.ds(me * own + step * sb, sb), 0:1].astype(jnp.int32)
        return degree_coefs(waves, count)

    def transform(step, coefs, slots):
        for s in slots:
            slot = step * sb + s
            zd = jnp.concatenate([zeta_ref[slot], delta_ref[slot]], axis=0)
            out = slot_fourier(values_ref[slot], *(c[s : s + 1] for c in coefs), zd)
            sums[pl.ds(s, rows, sb), :] = out

    def await_part(step, part):
        for copy in fetch(step, part):
            copy.wait()

    def legendre(step, first):
        if first:
            coefs = coefs_of(step)
            for part in range(pieces):
                await_part(step, part)
                if part == 0 and blocks > 2:
                    start_step(2)
                transform(step, coefs, range(part * piece, (part + 1) * piece))
        else:
            for part in range(pieces):
                await_part(step, part)
            pl.when(step + 2 < blocks)(lambda: start_step(step + 2))
            transform(step, coefs_of(step), range(sb))
        sent[:, step] = sums[...].astype(sent.dtype).reshape(rows, sb, columns)
        for cycle in range(cycles):
            mine = sums[pl.ds((me * cycles + cycle) * sb, sb), :]
            held[cycle, me, step] = mine.astype(held.dtype)

    legendre(0, True)
    pl.semaphore_wait(barrier, devices - 1)
    send(0, blocks == 1)

    def middle(step, carry):
        legendre(step, False)
        pl.when(step < blocks - 1)(lambda: send(step, False))
        pl.when(step == blocks - 1)(lambda: send(step, True))
        return carry

    lax.fori_loop(1, blocks, middle, 0)
    chunks = chunks_of(me, devices, blocks, sb)
    spans = []
    for sources, first, (low, high), _, _ in chunks:
        at = spans[-1].stop if spans else 0
        spans.append(slice(at, at + sources * (high - low) * sb))
        if high - low == blocks:
            wave_order[spans[-1]] = wave_col[pl.ds(first * own, sources * own)]
        else:
            for r in range(sources):
                size = (high - low) * sb
                wave_order[at + r * size : at + (r + 1) * size] = wave_col[
                    pl.ds((first + r) * own + low * sb, size)
                ]
    slots = wave_order.shape[0]
    wave_row = wave_order[...].T[0:1]
    for cycle in range(cycles):
        points = jnp.full((1, 1), points_ref[cycle], jnp.int32).astype(jnp.float32)
        cosine_sq = jnp.full((1, 1), cosine_ref[cycle], jnp.float32)
        fill_basis(wave_order, wave_row, points, basis)
        width = basis.shape[1]
        half = packed.shape[1] // 2
        for number, (sources, first, (low, high), slot, copies) in enumerate(chunks):
            span = spans[number]
            arriving = held.at[cycle, 0:copies, low:high]
            pltpu.make_async_copy(arriving, arriving, recv_sem.at[cycle, slot]).wait()
            arrived = held[cycle, pl.ds(first, sources), low:high].reshape(-1, columns)
            fill_fields(arrived, wave_row[:, span], points, cosine_sq, count, packed, span)
            for begin in range(0, width, 256):
                at = slice(begin, min(begin + 256, width))
                both = []
                for part in range(2):
                    x = jnp.dot(
                        packed[part, :, span],
                        basis[part * slots + span.start : part * slots + span.stop, at],
                        preferred_element_type=jnp.float32,
                    )
                    if number > 0:
                        x = total[part, :, at] + x
                    if number < len(chunks) - 1:
                        total[part, :, at] = x
                    both.append(x)
                if number == len(chunks) - 1:
                    cosine, sine = both
                    parts = (
                        cosine[:half] + sine[:half], cosine[half:] - sine[half:],
                        cosine[half:] + sine[half:], cosine[:half] - sine[:half],
                    )
                    for j, x in enumerate(parts):
                        quarters_ref[cycle, j * half : (j + 1) * half, at] = x.astype(quarters_ref.dtype)
    for cycle in range(cycles):
        others = held.at[cycle, 0 : devices - 1]
        pltpu.make_async_copy(others, others, send_sem.at[cycle]).wait()


def basis_width():
    return -(-(NLON // 4 + 1) // LANES) * LANES


def cycle_quarters(points, cosine_sq, wave_of_slot, vorticity, divergence, legendre):
    slots, half, count = vorticity.shape
    lines = legendre.shape[1]
    cycles = points.shape[0]
    devices = lines // cycles
    columns = 4 * half
    rows = 6 * half
    width = basis_width()
    sb = slot_block(slots)
    blocks = slots // sb
    hbm = pl.BlockSpec(memory_space=pltpu.HBM)
    return pl.pallas_call(
        exchange_kernel,
        in_specs=[pl.BlockSpec(memory_space=pltpu.SMEM)] * 2 + [hbm] * 4,
        out_specs=pl.BlockSpec(memory_space=pltpu.VMEM),
        out_shape=jax.ShapeDtypeStruct((cycles, 2 * rows, width), jnp.bfloat16),
        scratch_shapes=[
            pltpu.VMEM(wave_of_slot.shape, jnp.int32),
            pltpu.VMEM((devices * slots, LANES), jnp.float32),
            pltpu.VMEM((devices * slots, LANES), jnp.float32),
            pltpu.VMEM(vorticity.shape, vorticity.dtype),
            pltpu.VMEM(divergence.shape, divergence.dtype),
            pltpu.VMEM(legendre.shape, legendre.dtype),
            pltpu.VMEM((lines * sb, columns), jnp.float32),
            pltpu.VMEM((lines, blocks, sb, columns), jnp.bfloat16),
            pltpu.VMEM((cycles, devices, blocks, sb, columns), jnp.bfloat16),
            pltpu.VMEM((2 * devices * slots, width), jnp.bfloat16),
            pltpu.VMEM((2, rows, devices * slots), jnp.bfloat16),
            pltpu.VMEM((2, rows, width), jnp.float32),
            pltpu.SemaphoreType.DMA,
            pltpu.SemaphoreType.DMA((3, blocks, 2)),
            pltpu.SemaphoreType.DMA((cycles,)),
            pltpu.SemaphoreType.DMA((cycles, 3)),
        ],
        compiler_params=pltpu.CompilerParams(
            collective_id=0, has_side_effects=True, vmem_limit_bytes=44 << 20
        ),
    )(points, cosine_sq, *(
        pltpu.with_memory_space_constraint(x, pltpu.HBM)
        for x in (wave_of_slot, vorticity, divergence, legendre)
    ))


def place(quarters, first, points, line):
    rows = line.shape[0]
    width = quarters.shape[1]
    field = quarters.shape[0] // 4
    tiles = width // LANES
    quarter = points // 4
    lane = lax.broadcasted_iota(jnp.int32, (rows, LANES), 1)
    for j in range(4):
        turned = j % 2
        offset = quarter * (j + 1) - (width - 1) if turned else quarter * j
        offset = offset + front_lanes(width)
        base = pl.multiple_of(offset // LANES * LANES, LANES)
        shift = offset - base
        source = lane - shift if not turned else shift - 1 - lane
        source = source & (LANES - 1)
        previous = jnp.zeros((rows, LANES), jnp.float32)
        for t in range(tiles + 1):
            rolled = jnp.zeros((rows, LANES), jnp.float32)
            if t < tiles:
                u = tiles - 1 - t if turned else t
                tile = quarters[pl.ds(first + j * field, rows), u * LANES : (u + 1) * LANES]
                point = lane + u * LANES
                keep = (point > 0) & (point <= quarter) if turned else point < quarter
                tile = jnp.where(keep, tile.astype(jnp.float32), 0.0)
                rolled = jnp.take_along_axis(tile, source, axis=1)
            moved = jnp.where(lane < shift, previous, rolled).astype(line.dtype)
            at = pl.ds(pl.multiple_of(base + t * LANES, LANES), LANES)
            line[:, at] = line[:, at] + moved
            previous = rolled


def front_lanes(width):
    return width + LANES


def place_kernel(points_ref, quarters_ref, out_ref, line):
    cycle = pl.program_id(0)
    points = points_ref[cycle]
    line[...] = jnp.zeros_like(line)
    first = pl.multiple_of(pl.program_id(1) * line.shape[0], line.shape[0])
    place(quarters_ref.at[cycle], first, points, line)
    front = front_lanes(quarters_ref.shape[2])
    out_ref[0] = line[:, front : front + out_ref.shape[2]]


def row_block(rows):
    return rows


def placed(quarters, points):
    cycles, rows, width = quarters.shape
    rows = rows // 4
    step = row_block(rows)
    line = front_lanes(width) + 4 * width + 2 * LANES
    vmem = pl.BlockSpec(memory_space=pltpu.VMEM)
    return pl.pallas_call(
        place_kernel,
        grid=(cycles, rows // step),
        in_specs=[pl.BlockSpec(memory_space=pltpu.SMEM), vmem],
        out_specs=pl.BlockSpec((1, step, NLON), lambda i, k: (i, k, 0)),
        out_shape=jax.ShapeDtypeStruct((cycles, rows, NLON), jnp.bfloat16),
        scratch_shapes=[pltpu.VMEM((step, line), jnp.bfloat16)],
        compiler_params=pltpu.CompilerParams(vmem_limit_bytes=16 << 20),
    )(points, quarters)


def body(vorticity, divergence, legendre, wave_of_slot, cycle_points, cos_squared):
    quarters = cycle_quarters(
        cycle_points, cos_squared, wave_of_slot, vorticity, divergence, legendre
    )
    return placed(quarters, cycle_points)


def solution(mesh):
    return jax.shard_map(
        body,
        mesh=mesh,
        in_specs=(
            P(("member", "wave"), None, None),
            P(("member", "wave"), None, None),
            P("wave", None, None),
            P(),
            P("wave"),
            P("wave"),
        ),
        out_specs=P(("member", "wave"), None, None),
        check_vma=False,
    )
```
